32 devices in a mesh: grp: 4 (over y, core), rep: 8 (over z, x).
Axes of the slice: x: 2, y: 2, z: 4, core: 2. Of those that a mesh axis runs over, the one named last changes fastest.
Arguments:
- embeddings: bfloat16 [16384, 768], P(('grp', 'rep')), may hold values from -6 to 6
- cluster_ids: int32 [16384], P(('grp', 'rep')), may hold values from 0 to 12287, as said below
- owner_bounds: int32 [32], replicated, may hold values from 0 to 12287, as said below
Outputs:
- distance: float32 [16384], P(('grp', 'rep'))
- slot_index: int32 [16384], P(('grp', 'rep'))
- centroids: bfloat16 [32, 576, 768], P(('grp', 'rep'))
The draws below stay inside these ranges and needn't reach their ends.
Inputs may be any that keep to these rules, and one draw needn't show every extreme that they name: `cluster_ids`: in the rows of one device at most 48 rows belong to the clusters of one owner (owner o holds clusters owner_bounds[o] up to the next bound); in every draw some owner gets exactly 48 rows from every device. `owner_bounds`: owners are ordered grp first, then rep. The bounds rise from 0; each owner holds from 192 to 576 clusters, the last owner ending at 12288; some owner holds exactly 576.
All inputs are finite; a program needn't handle non-finite values.
Results may differ from the reference program's by a relative error of at most 0.004.
Values may be sent and summed in bfloat16 or wider, within the bound.
No kernel may reach another device: no remote copies, remote signals or barrier semaphores. Data moves between devices by JAX's collectives and lax.ppermute only.
A program may use at most 128 MiB of HBM per device.

```python
import jax
import jax.numpy as jnp
from jax import lax

D = 768
ROWS_DEV = 512
CL_DEV = 384
OWNERS = 32
ROWS = 16384
SLOT = 48
OWN_MAX = 576


def owner_layout(key):
    half_count = OWNERS // 2
    spread = CL_DEV // 2
    base_key = jax.random.fold_in(key, 11)
    first_key, second_key, third_key, fourth_key = jax.random.split(base_key, 4)
    deltas = jax.random.randint(first_key, (half_count,), -spread, spread + 1)
    chosen = jax.random.randint(second_key, (), 0, half_count)
    deltas = jnp.where(jnp.arange(half_count) == chosen, spread, deltas)
    widths = jnp.concatenate([CL_DEV + deltas, CL_DEV - deltas]).astype(jnp.int32)
    widths = jax.random.permutation(third_key, widths)
    bounds = (jnp.cumsum(widths) - widths).astype(jnp.int32)
    busy_owner = jax.random.randint(fourth_key, (), 0, OWNERS).astype(jnp.int32)
    return (bounds, widths, busy_owner)


def draw_owner_bounds(key, part):
    return owner_layout(key)[0]


def draw_cluster_ids(key, part):
    bounds, widths, busy_owner = owner_layout(key)
    pool_size = (OWNERS - 1) * (SLOT - 1)

    def one_device(device_index):
        device_key = jax.random.fold_in(jax.random.fold_in(key, 23), device_index)
        first_key, second_key, third_key = jax.random.split(device_key, 3)
        owner_pool = jnp.arange(pool_size, dtype=jnp.int32) % (OWNERS - 1)
        chosen = jax.random.permutation(first_key, owner_pool)[:ROWS_DEV - SLOT]
        chosen = chosen + (chosen >= busy_owner).astype(jnp.int32)
        owner_of = jnp.concatenate([jnp.full((SLOT,), busy_owner, jnp.int32), chosen])
        offsets = jax.random.randint(second_key, (ROWS_DEV,), 0, 1 << 30) % widths[owner_of]
        identity = (bounds[owner_of] + offsets).astype(jnp.int32)
        return jax.random.permutation(third_key, identity)
    return jax.vmap(one_device)(jnp.arange(OWNERS)).reshape(-1)


def block_scale(rng, shape, shards, smallest, top_value):
    factor_of = 1.0
    for axis_at, shards_of in shards:
        heights = jax.random.uniform(jax.random.fold_in(jax.random.fold_in(rng, 6), axis_at), (shards_of,), jnp.float32, smallest / len(shards), top_value / len(shards))
        factor_of = factor_of * jnp.repeat(jnp.exp(heights), shape[axis_at] // shards_of).reshape((-1,) + (1,) * (len(shape) - 1 - axis_at))
    return factor_of


def noise(own_key, extent, deviation, bound, cuts=(), kind=jnp.bfloat16):
    array = deviation * jax.random.normal(own_key, extent, jnp.float32)
    if cuts:
        array = array * block_scale(own_key, extent, cuts, -0.22, 0.18)
    return jnp.clip(array, -bound, bound).astype(kind)


def setup_inputs(seed: int = 0) -> dict:
    key_list = jax.random.split(jax.random.key(seed), 4)
    embeddings = noise(key_list[0], (ROWS, D), 1.0, 6.0, ((0, 32),))
    cluster_ids = draw_cluster_ids(jax.random.fold_in(key_list[3], 71), 0)
    owner_bounds = draw_owner_bounds(jax.random.fold_in(key_list[3], 71), 0)
    return dict(embeddings=embeddings, cluster_ids=cluster_ids, owner_bounds=owner_bounds)


epsilon = 1e-06
norm_floor = 0.25

def normalize(block):
    values = block.astype(jnp.float32)
    return (values * lax.rsqrt(lax.optimization_barrier(jnp.sum(values * values, axis=1, keepdims=True)) + epsilon)).astype(jnp.bfloat16)

def reference(embeddings, cluster_ids, owner_bounds):
    clusters = CL_DEV * OWNERS
    row_count = embeddings.shape[0]
    unit_blocks = lax.map(normalize, embeddings.reshape(OWNERS, ROWS_DEV, D))
    id_blocks = cluster_ids.reshape(OWNERS, ROWS_DEV)

    def accumulate(block, carry):
        block_rows = lax.dynamic_index_in_dim(unit_blocks, block, 0, keepdims=False)
        block_ids = lax.dynamic_index_in_dim(id_blocks, block, 0, keepdims=False)
        return carry + jax.ops.segment_sum(block_rows.astype(jnp.float32), block_ids, num_segments=clusters)
    member_sums = lax.fori_loop(0, OWNERS, accumulate, jnp.zeros((clusters, D), jnp.float32))
    members = jax.ops.segment_sum(jnp.ones((row_count,), jnp.float32), cluster_ids, num_segments=clusters)
    centroid = member_sums / jnp.maximum(members, 1.0)[:, None]
    centroid_norm = jnp.sqrt(lax.optimization_barrier(jnp.sum(centroid * centroid, axis=1)))
    unit_centroid = (centroid / jnp.maximum(centroid_norm, norm_floor)[:, None]).astype(jnp.bfloat16)

    def measure(pair):
        block_rows, block_ids = pair
        picked = unit_centroid[block_ids]
        return 1.0 - lax.optimization_barrier(jnp.sum(block_rows.astype(jnp.float32) * picked.astype(jnp.float32), axis=1))
    distance = lax.map(measure, (unit_blocks, id_blocks)).reshape(-1)
    sorted_rows = jnp.argsort(cluster_ids, stable=True).astype(jnp.int32)
    sorted_place = jnp.zeros((row_count,), jnp.int32).at[sorted_rows].set(jnp.arange(row_count, dtype=jnp.int32))
    sorted_ids = cluster_ids[sorted_rows]
    slot_index = (sorted_place - jnp.searchsorted(sorted_ids, cluster_ids, side='left').astype(jnp.int32)).astype(jnp.int32)
    range_ends = jnp.concatenate([owner_bounds[1:], jnp.full((1,), clusters, jnp.int32)])
    wanted = owner_bounds[:, None] + jnp.arange(OWN_MAX, dtype=jnp.int32)[None, :]
    inside = wanted < range_ends[:, None]
    table = unit_centroid[jnp.minimum(wanted, clusters - 1)]
    centroids = jnp.where(inside[:, :, None], table, jnp.zeros_like(table)).astype(jnp.bfloat16)
    return (distance, slot_index, centroids)
```

```python
import jax
import jax.numpy as jnp
from jax import lax
from jax.sharding import PartitionSpec as P

CL_DEV = 384


epsilon = 1e-06
norm_floor = 0.25
axes = ("grp", "rep")


def exchange(part):
    return lax.all_to_all(part, axes, split_axis=0, concat_axis=0, tiled=True)


def shards(embeddings, cluster_ids, owner_bounds):
    groups = lax.axis_size("grp")
    replicas = lax.axis_size("rep")
    owner_total = groups * replicas
    position = lax.axis_index("grp") * replicas + lax.axis_index("rep")
    row_count = embeddings.shape[0]
    feature_count = embeddings.shape[1]
    slot_count = 3 * row_count // owner_total
    owner_limit = CL_DEV + CL_DEV // 2
    places = owner_total * slot_count
    row_range = jnp.arange(row_count, dtype=jnp.int32)
    place_range = jnp.arange(places, dtype=jnp.int32)

    owner_of = jnp.sum(owner_bounds[None, :] <= cluster_ids[:, None], axis=1, dtype=jnp.int32) - 1
    earlier = (owner_of[:, None] == owner_of[None, :]) & (row_range[None, :] < row_range[:, None])
    target = owner_of * slot_count + jnp.sum(earlier, axis=1, dtype=jnp.int32)
    placed = place_range[:, None] == target[None, :]
    send_ids = jnp.sum(jnp.where(placed, cluster_ids[None, :] + 1, 0), axis=1, dtype=jnp.int32) - 1
    flat_ids = exchange(send_ids.reshape(owner_total, slot_count)).reshape(-1)

    values = embeddings.astype(jnp.float32)
    unit_rows = (
        values * lax.rsqrt(jnp.sum(values * values, axis=1, keepdims=True) + epsilon)
    ).astype(jnp.bfloat16)
    send_rows = jnp.dot(
        placed.astype(jnp.bfloat16), unit_rows, preferred_element_type=jnp.float32
    ).astype(jnp.bfloat16)
    flat_rows = exchange(send_rows.reshape(owner_total, slot_count, feature_count)).reshape(
        places, feature_count
    )

    twins = (flat_ids[:, None] == flat_ids[None, :]) & (place_range[None, :] < place_range[:, None])
    rank = jnp.sum(twins, axis=1, dtype=jnp.int32)
    local_index = flat_ids - owner_bounds[position]
    membership = jnp.arange(owner_limit, dtype=jnp.int32)[:, None] == local_index[None, :]
    members = jnp.sum(membership, axis=1, dtype=jnp.float32)
    member_sums = jnp.dot(
        membership.astype(jnp.bfloat16), flat_rows, preferred_element_type=jnp.float32
    )
    centroid = member_sums / jnp.maximum(members, 1.0)[:, None]
    centroid_norm = jnp.sqrt(jnp.sum(centroid * centroid, axis=1))
    unit_centroid = (centroid / jnp.maximum(centroid_norm, norm_floor)[:, None]).astype(
        jnp.bfloat16
    )
    products = lax.dot_general(
        unit_centroid, flat_rows, (((1,), (1,)), ((), ())), preferred_element_type=jnp.float32
    )
    owner_distance = 1.0 - jnp.sum(jnp.where(membership, products, 0.0), axis=0)
    answers = jnp.concatenate(
        [
            owner_distance.reshape(owner_total, slot_count),
            rank.astype(jnp.float32).reshape(owner_total, slot_count),
        ],
        axis=1,
    )
    returned = exchange(answers)
    mine = target[:, None] == place_range[None, :]
    distance = jnp.sum(jnp.where(mine, returned[:, :slot_count].reshape(1, -1), 0.0), axis=1)
    local_slot = jnp.sum(
        jnp.where(mine, returned[:, slot_count:].reshape(1, -1), 0.0), axis=1
    ).astype(jnp.int32)
    return (distance, local_slot, unit_centroid[None])


def solution(mesh):
    placed = (P(axes, None), P(axes), P())
    return jax.shard_map(
        shards,
        mesh=mesh,
        in_specs=placed,
        out_specs=(P(axes), P(axes), P(axes, None, None)),
        check_vma=False,
    )
```

```python
import jax
import jax.numpy as jnp
from jax import lax
from jax.sharding import PartitionSpec as P

CL_DEV = 384


epsilon = 1e-06
norm_floor = 0.25
axes = ("grp", "rep")


def exchange(part):
    return lax.all_to_all(part, axes, split_axis=0, concat_axis=0, tiled=True)


def shards(embeddings, cluster_ids, owner_bounds):
    groups = lax.axis_size("grp")
    replicas = lax.axis_size("rep")
    owner_total = groups * replicas
    position = lax.axis_index("grp") * replicas + lax.axis_index("rep")
    row_count = embeddings.shape[0]
    feature_count = embeddings.shape[1]
    slot_count = 3 * row_count // owner_total
    owner_limit = CL_DEV + CL_DEV // 2
    places = owner_total * slot_count
    row_range = jnp.arange(row_count, dtype=jnp.int32)
    place_range = jnp.arange(places, dtype=jnp.int32)

    owner_of = jnp.sum(owner_bounds[None, :] <= cluster_ids[:, None], axis=1, dtype=jnp.int32) - 1
    earlier = (owner_of[:, None] == owner_of[None, :]) & (row_range[None, :] < row_range[:, None])
    target = owner_of * slot_count + jnp.sum(earlier, axis=1, dtype=jnp.int32)
    placed = place_range[:, None] == target[None, :]
    send_ids = jnp.sum(jnp.where(placed, cluster_ids[None, :] + 1, 0), axis=1, dtype=jnp.int32) - 1
    values = embeddings.astype(jnp.float32)
    unit_rows = (
        values * lax.rsqrt(jnp.sum(values * values, axis=1, keepdims=True) + epsilon)
    ).astype(jnp.bfloat16)
    send_rows = jnp.dot(
        placed.astype(jnp.bfloat16), unit_rows, preferred_element_type=jnp.float32
    ).astype(jnp.bfloat16)
    send_rows, send_ids = lax.optimization_barrier((send_rows, send_ids))
    with jax.named_scope("rows"):
        flat_rows = exchange(send_rows.reshape(owner_total, slot_count, feature_count)).reshape(
            places, feature_count
        )
    with jax.named_scope("ids"):
        flat_ids = exchange(send_ids.reshape(owner_total, slot_count)).reshape(-1)

    twins = (flat_ids[:, None] == flat_ids[None, :]) & (place_range[None, :] < place_range[:, None])
    rank = jnp.sum(twins, axis=1, dtype=jnp.int32)
    local_index = flat_ids - owner_bounds[position]
    membership = jnp.arange(owner_limit, dtype=jnp.int32)[:, None] == local_index[None, :]
    members = jnp.sum(membership, axis=1, dtype=jnp.float32)
    member_sums = jnp.dot(
        membership.astype(jnp.bfloat16), flat_rows, preferred_element_type=jnp.float32
    )
    centroid = member_sums / jnp.maximum(members, 1.0)[:, None]
    centroid_norm = jnp.sqrt(jnp.sum(centroid * centroid, axis=1))
    unit_centroid = (centroid / jnp.maximum(centroid_norm, norm_floor)[:, None]).astype(
        jnp.bfloat16
    )
    products = lax.dot_general(
        unit_centroid, flat_rows, (((1,), (1,)), ((), ())), preferred_element_type=jnp.float32
    )
    owner_distance = 1.0 - jnp.sum(jnp.where(membership, products, 0.0), axis=0)
    answers = jnp.concatenate(
        [
            owner_distance.reshape(owner_total, slot_count),
            rank.astype(jnp.float32).reshape(owner_total, slot_count),
        ],
        axis=1,
    )
    returned = exchange(answers)
    mine = target[:, None] == place_range[None, :]
    distance = jnp.sum(jnp.where(mine, returned[:, :slot_count].reshape(1, -1), 0.0), axis=1)
    local_slot = jnp.sum(
        jnp.where(mine, returned[:, slot_count:].reshape(1, -1), 0.0), axis=1
    ).astype(jnp.int32)
    return (distance, local_slot, unit_centroid[None])


def solution(mesh):
    placed = (P(axes, None), P(axes), P())
    return jax.shard_map(
        shards,
        mesh=mesh,
        in_specs=placed,
        out_specs=(P(axes), P(axes), P(axes, None, None)),
        check_vma=False,
    )
```

```python
import jax
import jax.numpy as jnp
from jax import lax
from jax.sharding import PartitionSpec as P

CL_DEV = 384


epsilon = 1e-06
norm_floor = 0.25
axes = ("grp", "rep")


def exchange(part):
    return lax.all_to_all(part, axes, split_axis=0, concat_axis=0, tiled=True)


def shards(embeddings, cluster_ids, owner_bounds):
    groups = lax.axis_size("grp")
    replicas = lax.axis_size("rep")
    owner_total = groups * replicas
    position = lax.axis_index("grp") * replicas + lax.axis_index("rep")
    row_count = embeddings.shape[0]
    feature_count = embeddings.shape[1]
    slot_count = 3 * row_count // owner_total
    owner_limit = CL_DEV + CL_DEV // 2
    places = owner_total * slot_count
    row_range = jnp.arange(row_count, dtype=jnp.int32)
    place_range = jnp.arange(places, dtype=jnp.int32)

    owner_of = jnp.sum(owner_bounds[None, :] <= cluster_ids[:, None], axis=1, dtype=jnp.int32) - 1
    earlier = (owner_of[:, None] == owner_of[None, :]) & (row_range[None, :] < row_range[:, None])
    target = owner_of * slot_count + jnp.sum(earlier, axis=1, dtype=jnp.int32)
    placed = place_range[:, None] == target[None, :]
    values = embeddings.astype(jnp.float32)
    unit_rows = (
        values * lax.rsqrt(jnp.sum(values * values, axis=1, keepdims=True) + epsilon)
    ).astype(jnp.bfloat16)
    send_rows = jnp.dot(
        placed.astype(jnp.bfloat16), unit_rows, preferred_element_type=jnp.float32
    ).astype(jnp.bfloat16)
    send_rows, own_ids = lax.optimization_barrier((send_rows, cluster_ids))
    with jax.named_scope("rows"):
        flat_rows = exchange(send_rows.reshape(owner_total, slot_count, feature_count)).reshape(
            places, feature_count
        )
    with jax.named_scope("ids"):
        every_id = lax.all_gather(own_ids, axes, tiled=False)

    flat_every = every_id.reshape(1, -1)
    every_range = jnp.arange(owner_total * row_count, dtype=jnp.int32)[None, :]
    local_slot = jnp.sum(
        (flat_every == cluster_ids[:, None])
        & (every_range < (position * row_count + row_range)[:, None]),
        axis=1,
        dtype=jnp.int32,
    )
    first = owner_bounds[position]
    beyond = jnp.sum(jnp.where(jnp.arange(owner_total) == position + 1, owner_bounds, 0))
    beyond = jnp.where(position + 1 < owner_total, beyond, CL_DEV * owner_total)
    owned = (every_id >= first) & (every_id < beyond)
    upper = (row_range[:, None] < row_range[None, :]).astype(jnp.bfloat16)
    place_in = jnp.dot(
        owned.astype(jnp.bfloat16), upper, preferred_element_type=jnp.float32
    ).astype(jnp.int32)
    place_in = jnp.where(owned, place_in, -1)
    slot_range = jnp.arange(slot_count, dtype=jnp.int32)
    flat_ids = (
        jnp.sum(
            jnp.where(
                place_in[:, None, :] == slot_range[None, :, None], every_id[:, None, :] + 1, 0
            ),
            axis=2,
            dtype=jnp.int32,
        ).reshape(-1)
        - 1
    )
    local_index = flat_ids - owner_bounds[position]
    membership = jnp.arange(owner_limit, dtype=jnp.int32)[:, None] == local_index[None, :]
    members = jnp.sum(membership, axis=1, dtype=jnp.float32)
    member_sums = jnp.dot(
        membership.astype(jnp.bfloat16), flat_rows, preferred_element_type=jnp.float32
    )
    centroid = member_sums / jnp.maximum(members, 1.0)[:, None]
    centroid_norm = jnp.sqrt(jnp.sum(centroid * centroid, axis=1))
    unit_centroid = (centroid / jnp.maximum(centroid_norm, norm_floor)[:, None]).astype(
        jnp.bfloat16
    )
    products = lax.dot_general(
        unit_centroid, flat_rows, (((1,), (1,)), ((), ())), preferred_element_type=jnp.float32
    )
    owner_distance = 1.0 - jnp.sum(jnp.where(membership, products, 0.0), axis=0)
    returned = exchange(owner_distance.reshape(owner_total, slot_count)).reshape(1, -1)
    mine = target[:, None] == place_range[None, :]
    distance = jnp.sum(jnp.where(mine, returned, 0.0), axis=1)
    return (distance, local_slot, unit_centroid[None])


def solution(mesh):
    placed = (P(axes, None), P(axes), P())
    return jax.shard_map(
        shards,
        mesh=mesh,
        in_specs=placed,
        out_specs=(P(axes), P(axes), P(axes, None, None)),
        check_vma=False,
    )
```

```python
import jax
import jax.numpy as jnp
from jax import lax
from jax.sharding import PartitionSpec as P

CL_DEV = 384


epsilon = 1e-06
norm_floor = 0.25
axes = ("grp", "rep")


def exchange(part):
    return lax.all_to_all(part, axes, split_axis=0, concat_axis=0, tiled=True)


def shards(embeddings, cluster_ids, owner_bounds):
    groups = lax.axis_size("grp")
    replicas = lax.axis_size("rep")
    owner_total = groups * replicas
    position = lax.axis_index("grp") * replicas + lax.axis_index("rep")
    row_count = embeddings.shape[0]
    feature_count = embeddings.shape[1]
    slot_count = 3 * row_count // owner_total
    owner_limit = CL_DEV + CL_DEV // 2
    places = owner_total * slot_count
    row_range = jnp.arange(row_count, dtype=jnp.int32)
    place_range = jnp.arange(places, dtype=jnp.int32)

    owner_of = jnp.sum(owner_bounds[None, :] <= cluster_ids[:, None], axis=1, dtype=jnp.int32) - 1
    earlier = (owner_of[:, None] == owner_of[None, :]) & (row_range[None, :] < row_range[:, None])
    target = owner_of * slot_count + jnp.sum(earlier, axis=1, dtype=jnp.int32)
    placed = place_range[:, None] == target[None, :]
    send_ids = jnp.sum(jnp.where(placed, cluster_ids[None, :] + 1, 0), axis=1, dtype=jnp.int32)
    flat_ids = exchange(send_ids.reshape(owner_total, slot_count)).reshape(-1)

    values = embeddings.astype(jnp.float32)
    unit_rows = (
        values * lax.rsqrt(jnp.sum(values * values, axis=1, keepdims=True) + epsilon)
    ).astype(jnp.bfloat16)
    send_rows = jnp.dot(
        placed.astype(jnp.bfloat16), unit_rows, preferred_element_type=jnp.float32
    ).astype(jnp.bfloat16)
    flat_rows = exchange(send_rows.reshape(owner_total, slot_count, feature_count)).reshape(
        places, feature_count
    )

    twins = (flat_ids[:, None] == flat_ids[None, :]) & (place_range[None, :] < place_range[:, None])
    rank = jnp.sum(twins, axis=1, dtype=jnp.int32)
    local_index = flat_ids - (owner_bounds[position] + 1)
    membership = jnp.arange(owner_limit, dtype=jnp.int32)[:, None] == local_index[None, :]
    members = jnp.sum(membership, axis=1, dtype=jnp.float32)
    member_sums = jnp.dot(
        membership.astype(jnp.bfloat16), flat_rows, preferred_element_type=jnp.float32
    )
    centroid = member_sums / jnp.maximum(members, 1.0)[:, None]
    centroid_norm = jnp.sqrt(jnp.sum(centroid * centroid, axis=1))
    unit_centroid = (centroid / jnp.maximum(centroid_norm, norm_floor)[:, None]).astype(
        jnp.bfloat16
    )
    products = lax.dot_general(
        unit_centroid, flat_rows, (((1,), (1,)), ((), ())), preferred_element_type=jnp.float32
    )
    owner_distance = 1.0 - jnp.sum(jnp.where(membership, products, 0.0), axis=0)
    answers = jnp.concatenate(
        [
            owner_distance.reshape(owner_total, slot_count),
            rank.astype(jnp.float32).reshape(owner_total, slot_count),
        ],
        axis=1,
    )
    returned = exchange(answers)
    mine = target[:, None] == place_range[None, :]
    distance = jnp.sum(jnp.where(mine, returned[:, :slot_count].reshape(1, -1), 0.0), axis=1)
    ranks = returned[:, slot_count:].astype(jnp.int32).reshape(1, -1)
    local_slot = jnp.sum(jnp.where(mine, ranks, 0), axis=1, dtype=jnp.int32)
    return (distance, local_slot, unit_centroid[None])


def solution(mesh):
    placed = (P(axes, None), P(axes), P())
    return jax.shard_map(
        shards,
        mesh=mesh,
        in_specs=placed,
        out_specs=(P(axes), P(axes), P(axes, None, None)),
        check_vma=False,
    )
```
